32 devices in a mesh: dp: 1 (over z), tp: 4 (over y), ep: 8 (over x, core).
Axes of the slice: x: 4, y: 4, z: 1, core: 2. Of those that a mesh axis runs over, the one named last changes fastest.
The devices are a block of a 4x4x8 slice.
Arguments:
- tokens: bfloat16 [65536, 768], P(('dp', 'ep'))
- grad_out: bfloat16 [65536, 768], P(('dp', 'ep'))
- w_router: bfloat16 [768, 32], replicated
- w_in: bfloat16 [32, 768, 3072], P('ep', None, 'tp')
- w_out: bfloat16 [32, 3072, 768], P('ep', 'tp')
- expert_ids: int32 [65536], P(('dp', 'ep'))
Outputs:
- output 1: bfloat16 [65536, 768], P(('dp', 'ep'))
- output 2: bfloat16 [65536, 768], P(('dp', 'ep'))
- output 3: float32 [32, 768, 3072], P(('dp', 'ep'), None, 'tp')
- output 4: float32 [32, 3072, 768], P(('dp', 'ep'), 'tp')
- output 5: float32 [768, 32], P('dp')
All inputs are finite; a program needn't handle non-finite values.
Results may differ from the reference program's by a relative error of at most 0.00680241.
Values are sent between devices in bfloat16 or wider.
A program may use at most 768 MiB of HBM per device.

```python
import jax
import jax.numpy as jnp
from jax import lax

D_MODEL = 768
D_FF = 3072
EXPERTS = 32
TOKENS_DEV = 8192
EP_RANKS = 8

CAPACITY = (6 * TOKENS_DEV + 5 * EXPERTS - 1) // (5 * EXPERTS)
N_TOKENS = EP_RANKS * TOKENS_DEV
N_SLOTS = EXPERTS * CAPACITY


def draw_routes(route_key):
    key_hot, key_order, key_rest = jax.random.split(route_key, 3)
    hot_expert = jax.random.randint(key_hot, (EP_RANKS, 1), 0, EXPERTS)
    rest_ids = jax.random.randint(key_rest, (EP_RANKS, TOKENS_DEV), 0, EXPERTS)
    order_keys = jax.random.split(key_order, EP_RANKS)
    rank_of = jax.vmap(lambda one_key: jax.random.permutation(one_key, TOKENS_DEV))(order_keys)
    hot_count = CAPACITY + CAPACITY // 2 + 1
    cover_ids = (rank_of - hot_count) % EXPERTS
    route_ids = jnp.where(rank_of < hot_count, hot_expert, jnp.where(rank_of < hot_count + EXPERTS, cover_ids, rest_ids))
    return route_ids.reshape(N_TOKENS).astype(jnp.int32)


def setup_inputs(seed: int = 0, part: int = 0) -> dict:
    part_key = jax.random.fold_in(jax.random.key(seed), part)
    rand_keys = jax.random.split(part_key, 3)
    weight_keys = jax.random.split(jax.random.key(seed + 1), 3)
    tokens = jax.random.normal(rand_keys[0], (N_TOKENS, D_MODEL), jnp.float32)
    grad_out = jax.random.normal(rand_keys[1], (N_TOKENS, D_MODEL), jnp.float32)
    w_router = jax.random.normal(weight_keys[0], (D_MODEL, EXPERTS), jnp.float32) * D_MODEL ** -0.5
    w_in = jax.random.normal(weight_keys[1], (EXPERTS, D_MODEL, D_FF), jnp.float32) * D_MODEL ** -0.5
    w_out = jax.random.normal(weight_keys[2], (EXPERTS, D_FF, D_MODEL), jnp.float32) * D_FF ** -0.5
    return {
        "tokens": tokens.astype(jnp.bfloat16),
        "grad_out": grad_out.astype(jnp.bfloat16),
        "w_router": w_router.astype(jnp.bfloat16),
        "w_in": w_in.astype(jnp.bfloat16),
        "w_out": w_out.astype(jnp.bfloat16),
        "expert_ids": draw_routes(rand_keys[2]),
    }


def dispatch(rows, slot_index):
    slot_buf = jnp.zeros((N_SLOTS + 1, D_MODEL), rows.dtype).at[slot_index].set(rows)
    return slot_buf[:N_SLOTS]


def combine(slot_buf, slot_index):
    padded = jnp.concatenate([slot_buf, jnp.zeros((1, D_MODEL), slot_buf.dtype)], axis=0)
    return jnp.take(padded, slot_index, axis=0)


def by_expert(source_bufs):
    return source_bufs.reshape(EP_RANKS, EXPERTS, CAPACITY, D_MODEL).transpose(1, 0, 2, 3).reshape(EXPERTS, EP_RANKS * CAPACITY, D_MODEL)


def by_source(expert_bufs):
    return expert_bufs.reshape(EXPERTS, EP_RANKS, CAPACITY, D_MODEL).transpose(1, 0, 2, 3).reshape(EP_RANKS, N_SLOTS, D_MODEL)


def expert_step(operands):
    slot_rows, dy_rows, w_in_e, w_out_e = operands
    pre_act = jnp.dot(slot_rows, w_in_e, preferred_element_type=jnp.float32)
    act_val, act_vjp = jax.vjp(jax.nn.gelu, pre_act)
    hidden = act_val.astype(jnp.bfloat16)
    y_rows = jnp.dot(hidden, w_out_e, preferred_element_type=jnp.float32).astype(jnp.bfloat16)
    d_hidden = jnp.dot(dy_rows, w_out_e.T, preferred_element_type=jnp.float32)
    d_pre = act_vjp(d_hidden)[0].astype(jnp.bfloat16)
    grad_out_e = jnp.dot(hidden.T, dy_rows, preferred_element_type=jnp.float32)
    grad_in_e = jnp.dot(slot_rows.T, d_pre, preferred_element_type=jnp.float32)
    d_slot = jnp.dot(d_pre, w_in_e.T, preferred_element_type=jnp.float32).astype(jnp.bfloat16)
    return y_rows, d_slot, grad_in_e, grad_out_e


def reference(tokens, grad_out, w_router, w_in, w_out, expert_ids):
    route_ids = expert_ids.reshape(EP_RANKS, TOKENS_DEV)
    one_hot = (route_ids[:, :, None] == jnp.arange(EXPERTS)[None, None, :]).astype(jnp.int32)
    position = jnp.sum(jnp.cumsum(one_hot, axis=1) * one_hot, axis=2) - 1
    slot_index = jnp.where(position < CAPACITY, route_ids * CAPACITY + position, N_SLOTS)
    chosen = expert_ids[:, None] == jnp.arange(EXPERTS)[None, :]
    logits = jnp.dot(tokens, w_router, preferred_element_type=jnp.float32)
    router_prob = jax.nn.softmax(logits, axis=-1)
    gate_prob = jnp.sum(jnp.where(chosen, router_prob, 0.0), axis=1)
    dy_tok = (gate_prob[:, None] * grad_out.astype(jnp.float32)).astype(jnp.bfloat16)
    slot_rows = jax.vmap(dispatch)(tokens.reshape(EP_RANKS, TOKENS_DEV, D_MODEL), slot_index)
    dy_rows = jax.vmap(dispatch)(dy_tok.reshape(EP_RANKS, TOKENS_DEV, D_MODEL), slot_index)
    y_rows, d_slot, grad_w_in, grad_w_out = lax.map(expert_step, (by_expert(slot_rows), by_expert(dy_rows), w_in, w_out))
    y_tok = jax.vmap(combine)(by_source(y_rows), slot_index).reshape(N_TOKENS, D_MODEL)
    dx_moe = jax.vmap(combine)(by_source(d_slot), slot_index).reshape(N_TOKENS, D_MODEL)
    moe_out = (gate_prob[:, None] * y_tok.astype(jnp.float32)).astype(jnp.bfloat16)
    d_gate = jnp.sum(grad_out.astype(jnp.float32) * y_tok.astype(jnp.float32), axis=1)
    d_logits = (d_gate[:, None] * router_prob * (chosen.astype(jnp.float32) - gate_prob[:, None])).astype(jnp.bfloat16)
    router_grad = jnp.dot(d_logits, w_router.T, preferred_element_type=jnp.float32)
    grad_tokens = (dx_moe.astype(jnp.float32) + router_grad).astype(jnp.bfloat16)
    grad_w_router = jnp.dot(tokens.T, d_logits, preferred_element_type=jnp.float32)
    return moe_out, grad_tokens, grad_w_in, grad_w_out, grad_w_router
```

```python
import jax
import jax.numpy as jnp
from jax import lax
from jax.sharding import PartitionSpec as P


def solution(mesh):
    ep_size = mesh.shape["ep"]
    tp_size = mesh.shape["tp"]
    row_spec = P(("dp", "ep"), None)
    bf16, f32 = jnp.bfloat16, jnp.float32

    def block(tokens, grad_out, w_router, w_in, w_out, expert_ids):
        n_local, _ = tokens.shape
        n_experts = w_router.shape[1]
        local_experts = w_in.shape[0]
        assert local_experts == tp_size == 4
        capacity = (6 * n_local + 5 * n_experts - 1) // (5 * n_experts)
        cap = (capacity + 7) // 8 * 8
        my_tp = lax.axis_index("tp")

        def from_offset(weight, offset):
            mine = lax.dynamic_index_in_dim(weight, (my_tp - offset) % tp_size, 0, keepdims=False)
            return lax.ppermute(mine, "tp", [(i, (i - offset) % tp_size) for i in range(tp_size)])

        def gather_weight(weight):
            own = lax.dynamic_index_in_dim(weight, my_tp, 0, keepdims=False)
            return jnp.stack([from_offset(weight, 2), own, from_offset(weight, 1), from_offset(weight, 3)])

        wi, wo = gather_weight(w_in), gather_weight(w_out)

        block = 256
        n_blocks = n_local // block
        chosen_t = jnp.arange(n_experts)[:, None] == expert_ids[None, :]
        upper = (jnp.arange(block)[:, None] <= jnp.arange(block)[None, :]).astype(bf16)
        one_hot = chosen_t.astype(bf16).reshape(n_experts * n_blocks, block)
        inside = jnp.dot(one_hot, upper, preferred_element_type=f32).reshape(n_experts, n_blocks, block)
        totals = inside[:, :, -1]
        before = jnp.dot(totals.astype(bf16), (jnp.arange(n_blocks)[:, None] < jnp.arange(n_blocks)[None, :]).astype(bf16), preferred_element_type=f32)
        running = (inside + before[:, :, None]).reshape(n_experts, n_local)
        position = (jnp.sum(jnp.where(chosen_t, running, 0.0), axis=0) - 1.0).astype(jnp.int32)
        kept = position < capacity

        token_ids = jnp.arange(n_local)
        at_slot = (jnp.where(kept, position, cap)[None, :] == jnp.arange(cap)[:, None]).astype(bf16)
        high = (token_ids // 128).astype(f32)
        low = (token_ids % 128).astype(f32)

        def slot_map(row):
            experts = jnp.arange(ep_size) * tp_size + row
            mine = expert_ids[None, :] == experts[:, None]
            digits = jnp.concatenate([jnp.where(mine, high, 0.0), jnp.where(mine, low, 0.0), mine.astype(f32)]).astype(bf16)
            found = lax.dot_general(digits, at_slot, (((1,), (1,)), ((), ())), preferred_element_type=f32).reshape(3, ep_size, cap)
            token = (found[0] * 128.0 + found[1]).astype(jnp.int32)
            filled = found[2] > 0.5
            token = jnp.where(filled, token, token[:, :1])
            return experts, token.reshape(-1), filled.reshape(-1)

        def exchange(rows):
            return lax.all_to_all(rows.reshape(ep_size, cap, rows.shape[1]), "ep", 0, 0, tiled=True).reshape(rows.shape)

        def send_rows(row):
            experts, slot_token, filled = slot_map(row)
            x_send = jnp.take(tokens, slot_token, axis=0, mode="clip")
            gy_send = jnp.take(grad_out, slot_token, axis=0, mode="clip")
            prob = jax.nn.softmax(jnp.dot(x_send, w_router, preferred_element_type=f32), axis=-1)
            slot_expert = jnp.repeat(experts, cap)
            gate = jnp.sum(jnp.where(slot_expert[:, None] == jnp.arange(n_experts)[None, :], prob, 0.0), axis=1)
            gate = jnp.where(filled, gate, 0.0)
            dy_send = (gate[:, None] * gy_send.astype(f32)).astype(bf16)
            return x_send, dy_send

        x_send, dy_send = send_rows(my_tp)
        x_rows = exchange(x_send)
        dy_rows = exchange(dy_send)

        pre_act = jnp.einsum("rd,kdf->krf", x_rows, wi, preferred_element_type=f32)
        act_val, act_vjp = jax.vjp(jax.nn.gelu, pre_act)
        hidden = act_val.astype(bf16)
        y_rows = jnp.einsum("krf,kfd->rd", hidden, wo, preferred_element_type=f32).astype(bf16)
        y_back = exchange(y_rows)
        y_all = lax.all_gather(y_back, "tp", axis=0, tiled=True)

        d_hidden = jnp.einsum("rd,kfd->krf", dy_rows, wo, preferred_element_type=f32)
        d_pre = act_vjp(d_hidden)[0].astype(bf16)
        d_slot = jnp.einsum("krf,kdf->rd", d_pre, wi, preferred_element_type=f32).astype(bf16)
        s_back = exchange(d_slot)
        s_all = lax.all_gather(s_back, "tp", axis=0, tiled=True)

        far_tp = (my_tp + 2) % tp_size
        far_x, far_dy = send_rows(far_tp)
        far_x = exchange(far_x)
        far_dy = exchange(far_dy)
        far_pre = jnp.dot(far_x, lax.dynamic_index_in_dim(w_in, far_tp, 0, keepdims=False), preferred_element_type=f32)
        far_act, far_vjp = jax.vjp(jax.nn.gelu, far_pre)
        far_hidden = far_act.astype(bf16)
        far_dh = lax.dot_general(far_dy, lax.dynamic_index_in_dim(w_out, far_tp, 0, keepdims=False), (((1,), (1,)), ((), ())), preferred_element_type=f32)
        far_dpre = far_vjp(far_dh)[0].astype(bf16)

        def rows_product(left, right):
            return lax.dot_general(left, right, (((0,), (0,)), ((), ())), preferred_element_type=f32)

        def spread(left, right, far_left, far_right):
            own, nxt, prv = [rows_product(left[k] if left.ndim == 3 else left, right[k] if right.ndim == 3 else right) for k in (1, 2, 3)]
            far = rows_product(far_left, far_right)
            up = lax.ppermute(nxt, "tp", [(i, (i + 1) % tp_size) for i in range(tp_size)])
            down = lax.ppermute(prv, "tp", [(i, (i - 1) % tp_size) for i in range(tp_size)])
            grads = jnp.zeros((local_experts,) + own.shape, f32)
            for part, offset in ((own, 0), (far, 2), (up, 3), (down, 1)):
                grads = lax.dynamic_update_index_in_dim(grads, part, (my_tp + offset) % tp_size, 0)
            return grads

        grad_w_out = spread(hidden, dy_rows, far_hidden, far_dy)
        grad_w_in = spread(x_rows, d_pre, far_x, far_dpre)

        logits = jnp.dot(tokens, w_router, preferred_element_type=f32)
        router_prob = jax.nn.softmax(logits, axis=-1)
        chosen = expert_ids[:, None] == jnp.arange(n_experts)[None, :]
        gate_prob = jnp.sum(jnp.where(chosen, router_prob, 0.0), axis=1)
        slot_row = ((expert_ids % tp_size) * ep_size + expert_ids // tp_size) * cap + jnp.minimum(position, cap - 1)
        y_tok = jnp.where(kept[:, None], jnp.take(y_all, slot_row, axis=0, mode="clip"), 0)
        dx_moe = jnp.where(kept[:, None], jnp.take(s_all, slot_row, axis=0, mode="clip"), 0)
        moe_out = (gate_prob[:, None] * y_tok.astype(f32)).astype(bf16)
        d_gate = jnp.sum(grad_out.astype(f32) * y_tok.astype(f32), axis=1)
        d_logits = (d_gate[:, None] * router_prob * (chosen.astype(f32) - gate_prob[:, None])).astype(bf16)
        router_grad = jnp.einsum("te,de->td", d_logits, w_router, preferred_element_type=f32)
        grad_tokens = (dx_moe.astype(f32) + router_grad).astype(bf16)
        grad_w_router = lax.psum(jnp.einsum("td,te->de", tokens, d_logits, preferred_element_type=f32), "ep")
        return moe_out, grad_tokens, grad_w_in, grad_w_out, grad_w_router

    in_specs = (row_spec, row_spec, P(None, None), P("ep", None, "tp"), P("ep", "tp", None), P(("dp", "ep")))
    out_specs = (row_spec, row_spec, P(("dp", "ep"), None, "tp"), P(("dp", "ep"), "tp", None), P("dp", None))
    return jax.shard_map(block, mesh=mesh, in_specs=in_specs, out_specs=out_specs, check_vma=False)
```

```python
import jax
import jax.numpy as jnp
from jax import lax
from jax.sharding import PartitionSpec as P


def solution(mesh):
    ep_size = mesh.shape["ep"]
    tp_size = mesh.shape["tp"]
    row_spec = P(("dp", "ep"), None)
    bf16, f32 = jnp.bfloat16, jnp.float32

    def gelu_and_slope(a):
        c, k = (2.0 / jnp.pi) ** 0.5, 0.044715
        square = a * a
        t = jnp.tanh(a * (c + (c * k) * square))
        half = 0.5 + 0.5 * t
        value = a * half
        return value.astype(bf16), half + value * (1.0 - t) * (c + (3.0 * c * k) * square)

    def block(tokens, grad_out, w_router, w_in, w_out, expert_ids):
        n_local, d_model = tokens.shape
        n_experts = w_router.shape[1]
        local_experts = w_in.shape[0]
        assert local_experts == tp_size == 4
        capacity = (6 * n_local + 5 * n_experts - 1) // (5 * n_experts)
        cap = (capacity + 7) // 8 * 8
        my_tp = lax.axis_index("tp")

        def from_offset(weight, offset):
            mine = lax.dynamic_index_in_dim(weight, (my_tp - offset) % tp_size, 0, keepdims=False)
            return lax.ppermute(mine, "tp", [(i, (i - offset) % tp_size) for i in range(tp_size)])

        def gather_weight(weight):
            own = lax.dynamic_index_in_dim(weight, my_tp, 0, keepdims=False)
            return jnp.stack([from_offset(weight, 2), own, from_offset(weight, 1), from_offset(weight, 3)])

        wi = gather_weight(w_in)
        wo = gather_weight(w_out)

        block = 256
        n_blocks = n_local // block
        chosen_t = jnp.arange(n_experts)[:, None] == expert_ids[None, :]
        upper = (jnp.arange(block)[:, None] <= jnp.arange(block)[None, :]).astype(bf16)
        one_hot = chosen_t.astype(bf16).reshape(n_experts * n_blocks, block)
        inside = jnp.dot(one_hot, upper, preferred_element_type=f32).reshape(n_experts, n_blocks, block)
        totals = inside[:, :, -1]
        before = jnp.dot(totals.astype(bf16), (jnp.arange(n_blocks)[:, None] < jnp.arange(n_blocks)[None, :]).astype(bf16), preferred_element_type=f32)
        running = (inside + before[:, :, None]).reshape(n_experts, n_local)
        position = (jnp.sum(jnp.where(chosen_t, running, 0.0), axis=0) - 1.0).astype(jnp.int32)
        kept = position < capacity

        token_ids = jnp.arange(n_local)
        at_slot = (jnp.where(kept, position, cap)[None, :] == jnp.arange(cap)[:, None]).astype(bf16)
        high = (token_ids // 128).astype(f32)
        low = (token_ids % 128).astype(f32)

        def slot_map(row):
            experts = jnp.arange(ep_size) * tp_size + row
            mine = expert_ids[None, :] == experts[:, None]
            digits = jnp.concatenate([jnp.where(mine, high, 0.0), jnp.where(mine, low, 0.0), mine.astype(f32)]).astype(bf16)
            found = lax.dot_general(digits, at_slot, (((1,), (1,)), ((), ())), preferred_element_type=f32).reshape(3, ep_size, cap)
            token = (found[0] * 128.0 + found[1]).astype(jnp.int32)
            filled = found[2] > 0.5
            token = jnp.where(filled, token, token[:, :1])
            return experts, token.reshape(-1), filled.reshape(-1)

        def exchange(rows):
            return lax.all_to_all(rows.reshape(ep_size, cap, rows.shape[1]), "ep", 0, 0, tiled=True).reshape(rows.shape)

        def send_rows(row):
            experts, slot_token, filled = slot_map(row)
            x_send = jnp.take(tokens, slot_token, axis=0, mode="clip")
            gy_send = jnp.take(grad_out, slot_token, axis=0, mode="clip")
            prob = jax.nn.softmax(jnp.dot(x_send, w_router, preferred_element_type=f32), axis=-1)
            slot_expert = jnp.repeat(experts, cap)
            gate = jnp.sum(jnp.where(slot_expert[:, None] == jnp.arange(n_experts)[None, :], prob, 0.0), axis=1)
            gate = jnp.where(filled, gate, 0.0)
            dy_send = (gate[:, None] * gy_send.astype(f32)).astype(bf16)
            return x_send, dy_send

        x_send, dy_send = send_rows(my_tp)
        x_rows = exchange(x_send)
        dy_rows = exchange(dy_send)

        pre_act = jnp.einsum("rd,kdf->krf", x_rows, wi, preferred_element_type=f32)
        hidden, slope = gelu_and_slope(pre_act)
        y_rows = jnp.einsum("krf,kfd->rd", hidden, wo, preferred_element_type=f32).astype(bf16)
        early = d_model // 3
        y_early = lax.all_gather(y_rows[:, :early], "tp", axis=0, tiled=True).reshape(tp_size, ep_size, cap, early)
        y_back = exchange(y_rows[:, early:])
        y_all = lax.all_gather(y_back, "tp", axis=0, tiled=True)
        y_early = lax.all_to_all(y_early, "ep", 1, 1, tiled=True).reshape(-1, early)

        d_hidden = jnp.einsum("rd,kfd->krf", dy_rows, wo, preferred_element_type=f32)
        d_pre = (d_hidden * slope).astype(bf16)
        d_slot = jnp.einsum("krf,kdf->rd", d_pre, wi, preferred_element_type=f32).astype(bf16)
        s_back = exchange(d_slot)
        s_all = lax.all_gather(s_back, "tp", axis=0, tiled=True)

        far_tp = (my_tp + 2) % tp_size
        far_x, far_dy = send_rows(far_tp)
        far_x = exchange(far_x)
        far_dy = exchange(far_dy)
        far_pre = jnp.dot(far_x, lax.dynamic_index_in_dim(w_in, far_tp, 0, keepdims=False), preferred_element_type=f32)
        far_hidden, far_slope = gelu_and_slope(far_pre)
        far_dh = lax.dot_general(far_dy, lax.dynamic_index_in_dim(w_out, far_tp, 0, keepdims=False), (((1,), (1,)), ((), ())), preferred_element_type=f32)
        far_dpre = (far_dh * far_slope).astype(bf16)

        def rows_product(left, right):
            return lax.dot_general(left, right, (((0,), (0,)), ((), ())), preferred_element_type=f32)

        def spread(left, right, far_left, far_right):
            own, nxt, prv = [rows_product(left[k] if left.ndim == 3 else left, right[k] if right.ndim == 3 else right) for k in (1, 2, 3)]
            far = rows_product(far_left, far_right)
            up = lax.ppermute(nxt, "tp", [(i, (i + 1) % tp_size) for i in range(tp_size)])
            down = lax.ppermute(prv, "tp", [(i, (i - 1) % tp_size) for i in range(tp_size)])
            grads = jnp.zeros((local_experts,) + own.shape, f32)
            for part, offset in ((own, 0), (far, 2), (up, 3), (down, 1)):
                grads = lax.dynamic_update_index_in_dim(grads, part, (my_tp + offset) % tp_size, 0)
            return grads

        grad_w_out = spread(hidden, dy_rows, far_hidden, far_dy)
        grad_w_in = spread(x_rows, d_pre, far_x, far_dpre)

        logits = jnp.dot(tokens, w_router, preferred_element_type=f32)
        router_prob = jax.nn.softmax(logits, axis=-1)
        chosen = expert_ids[:, None] == jnp.arange(n_experts)[None, :]
        gate_prob = jnp.sum(jnp.where(chosen, router_prob, 0.0), axis=1)
        slot_row = ((expert_ids % tp_size) * ep_size + expert_ids // tp_size) * cap + jnp.minimum(position, cap - 1)
        y_all = jnp.concatenate([y_early, y_all], axis=1)
        y_tok = jnp.where(kept[:, None], jnp.take(y_all, slot_row, axis=0, mode="clip"), 0)
        dx_moe = jnp.where(kept[:, None], jnp.take(s_all, slot_row, axis=0, mode="clip"), 0)
        moe_out = (gate_prob[:, None] * y_tok.astype(f32)).astype(bf16)
        d_gate = jnp.sum(grad_out.astype(f32) * y_tok.astype(f32), axis=1)
        d_logits = (d_gate[:, None] * router_prob * (chosen.astype(f32) - gate_prob[:, None])).astype(bf16)
        router_grad = lax.dot_general(d_logits, w_router, (((1,), (1,)), ((), ())), preferred_element_type=f32)
        grad_tokens = (dx_moe.astype(f32) + router_grad).astype(bf16)
        grad_w_router = lax.psum(jnp.einsum("td,te->de", tokens, d_logits, preferred_element_type=f32), "ep")
        return moe_out, grad_tokens, grad_w_in, grad_w_out, grad_w_router

    in_specs = (row_spec, row_spec, P(None, None), P("ep", None, "tp"), P("ep", "tp", None), P(("dp", "ep")))
    out_specs = (row_spec, row_spec, P(("dp", "ep"), None, "tp"), P(("dp", "ep"), "tp", None), P("dp", None))
    return jax.shard_map(block, mesh=mesh, in_specs=in_specs, out_specs=out_specs, check_vma=False)
```

```python
import jax
import jax.numpy as jnp
from jax import lax
from jax.experimental import pallas as pl
from jax.sharding import PartitionSpec as P


def solution(mesh):
    ep_size = mesh.shape["ep"]
    tp_size = mesh.shape["tp"]
    row_spec = P(("dp", "ep"), None)
    bf16, f32 = jnp.bfloat16, jnp.float32

    def gelu_and_slope(a):
        c, k = (2.0 / jnp.pi) ** 0.5, 0.044715
        square = a * a
        t = jnp.tanh(a * (c + (c * k) * square))
        half = 0.5 + 0.5 * t
        value = a * half
        return value.astype(bf16), half + value * (1.0 - t) * (c + (3.0 * c * k) * square)

    def block(tokens, grad_out, w_router, w_in, w_out, expert_ids):
        n_local, d_model = tokens.shape
        n_experts = w_router.shape[1]
        local_experts = w_in.shape[0]
        assert local_experts == tp_size == 4
        capacity = (6 * n_local + 5 * n_experts - 1) // (5 * n_experts)
        cap = (capacity + 7) // 8 * 8
        my_tp = lax.axis_index("tp")

        def from_offset(weight, offset):
            mine = lax.dynamic_index_in_dim(weight, (my_tp - offset) % tp_size, 0, keepdims=False)
            return lax.ppermute(mine, "tp", [(i, (i - offset) % tp_size) for i in range(tp_size)])

        def gather_weight(weight):
            own = lax.dynamic_index_in_dim(weight, my_tp, 0, keepdims=False)
            return jnp.stack([from_offset(weight, 2), own, from_offset(weight, 1), from_offset(weight, 3)])

        wi = gather_weight(w_in)
        wo = gather_weight(w_out)

        block = 256
        n_blocks = n_local // block
        chosen_t = jnp.arange(n_experts)[:, None] == expert_ids[None, :]
        upper = (jnp.arange(block)[:, None] <= jnp.arange(block)[None, :]).astype(bf16)
        one_hot = chosen_t.astype(bf16).reshape(n_experts * n_blocks, block)
        inside = jnp.dot(one_hot, upper, preferred_element_type=f32).reshape(n_experts, n_blocks, block)
        totals = inside[:, :, -1]
        before = jnp.dot(totals.astype(bf16), (jnp.arange(n_blocks)[:, None] < jnp.arange(n_blocks)[None, :]).astype(bf16), preferred_element_type=f32)
        running = (inside + before[:, :, None]).reshape(n_experts, n_local)
        position = (jnp.sum(jnp.where(chosen_t, running, 0.0), axis=0) - 1.0).astype(jnp.int32)
        kept = position < capacity

        token_ids = jnp.arange(n_local)
        at_slot = (jnp.where(kept, position, cap)[None, :] == jnp.arange(cap)[:, None]).astype(bf16)
        high = (token_ids // 128).astype(f32)
        low = (token_ids % 128).astype(f32)

        def slot_map(row):
            experts = jnp.arange(ep_size) * tp_size + row
            mine = expert_ids[None, :] == experts[:, None]
            digits = jnp.concatenate([jnp.where(mine, high, 0.0), jnp.where(mine, low, 0.0), mine.astype(f32)]).astype(bf16)
            found = lax.dot_general(digits, at_slot, (((1,), (1,)), ((), ())), preferred_element_type=f32).reshape(3, ep_size, cap)
            token = (found[0] * 128.0 + found[1]).astype(jnp.int32)
            filled = found[2] > 0.5
            token = jnp.where(filled, token, token[:, :1])
            return experts, token.reshape(-1), filled.reshape(-1)

        def exchange(rows):
            return lax.all_to_all(rows.reshape(ep_size, cap, rows.shape[1]), "ep", 0, 0, tiled=True).reshape(rows.shape)

        def send_rows(row):
            experts, slot_token, filled = slot_map(row)
            x_send = jnp.take(tokens, slot_token, axis=0, mode="clip")
            gy_send = jnp.take(grad_out, slot_token, axis=0, mode="clip")
            prob = jax.nn.softmax(jnp.dot(x_send, w_router, preferred_element_type=f32), axis=-1)
            slot_expert = jnp.repeat(experts, cap)
            gate = jnp.sum(jnp.where(slot_expert[:, None] == jnp.arange(n_experts)[None, :], prob, 0.0), axis=1)
            gate = jnp.where(filled, gate, 0.0)
            dy_send = (gate[:, None] * gy_send.astype(f32)).astype(bf16)
            return x_send, dy_send

        x_send, dy_send = send_rows(my_tp)
        x_rows = exchange(x_send)
        dy_rows = exchange(dy_send)

        pre_act = jnp.einsum("rd,kdf->krf", x_rows, wi, preferred_element_type=f32)
        hidden, slope = gelu_and_slope(pre_act)
        early = d_model // 3

        def y_columns(part):
            return jnp.einsum("krf,kfd->rd", hidden, part, preferred_element_type=f32).astype(bf16)

        y_first = y_columns(wo[:, :, :early])
        y_rest = y_columns(wo[:, :, early:])
        y_early = lax.all_gather(y_first, "tp", axis=0, tiled=True).reshape(tp_size, ep_size, cap, early)
        y_back = exchange(y_rest)
        y_all = lax.all_gather(y_back, "tp", axis=0, tiled=True)
        y_early = lax.all_to_all(y_early, "ep", 1, 1, tiled=True).reshape(-1, early)

        d_hidden = jnp.einsum("rd,kfd->krf", dy_rows, wo, preferred_element_type=f32)
        d_pre = (d_hidden * slope).astype(bf16)
        d_slot = jnp.einsum("krf,kdf->rd", d_pre, wi, preferred_element_type=f32).astype(bf16)
        s_back = exchange(d_slot)
        s_all = lax.all_gather(s_back, "tp", axis=0, tiled=True)

        far_tp = (my_tp + 2) % tp_size
        far_x, far_dy = send_rows(far_tp)
        far_x = exchange(far_x)
        far_dy = exchange(far_dy)
        far_pre = jnp.dot(far_x, lax.dynamic_index_in_dim(w_in, far_tp, 0, keepdims=False), preferred_element_type=f32)
        far_hidden, far_slope = gelu_and_slope(far_pre)
        far_dh = lax.dot_general(far_dy, lax.dynamic_index_in_dim(w_out, far_tp, 0, keepdims=False), (((1,), (1,)), ((), ())), preferred_element_type=f32)
        far_dpre = (far_dh * far_slope).astype(bf16)

        def rows_product(left, right):
            return lax.dot_general(left, right, (((0,), (0,)), ((), ())), preferred_element_type=f32)

        def spread(left, right, far_left, far_right):
            own, nxt, prv = [rows_product(left[k] if left.ndim == 3 else left, right[k] if right.ndim == 3 else right) for k in (1, 2, 3)]
            far = rows_product(far_left, far_right)
            up = lax.ppermute(nxt, "tp", [(i, (i + 1) % tp_size) for i in range(tp_size)])
            down = lax.ppermute(prv, "tp", [(i, (i - 1) % tp_size) for i in range(tp_size)])
            grads = pl.pallas_call(
                lambda ref: None,
                out_shape=jax.ShapeDtypeStruct((local_experts,) + own.shape, f32),
                out_specs=pl.BlockSpec(memory_space=pl.ANY),
            )()
            for part, offset in ((own, 0), (far, 2), (up, 3), (down, 1)):
                grads = lax.dynamic_update_index_in_dim(grads, part, (my_tp + offset) % tp_size, 0)
            return grads

        grad_w_out = spread(hidden, dy_rows, far_hidden, far_dy)
        grad_w_in = spread(x_rows, d_pre, far_x, far_dpre)

        logits = jnp.dot(tokens, w_router, preferred_element_type=f32)
        router_prob = jax.nn.softmax(logits, axis=-1)
        chosen = expert_ids[:, None] == jnp.arange(n_experts)[None, :]
        gate_prob = jnp.sum(jnp.where(chosen, router_prob, 0.0), axis=1)
        slot_row = ((expert_ids % tp_size) * ep_size + expert_ids // tp_size) * cap + jnp.minimum(position, cap - 1)
        y_all = jnp.concatenate([y_early, y_all], axis=1)
        y_tok = jnp.where(kept[:, None], jnp.take(y_all, slot_row, axis=0, mode="clip"), 0)
        dx_moe = jnp.where(kept[:, None], jnp.take(s_all, slot_row, axis=0, mode="clip"), 0)
        moe_out = (gate_prob[:, None] * y_tok.astype(f32)).astype(bf16)
        d_gate = jnp.sum(grad_out.astype(f32) * y_tok.astype(f32), axis=1)
        d_logits = (d_gate[:, None] * router_prob * (chosen.astype(f32) - gate_prob[:, None])).astype(bf16)
        router_grad = lax.dot_general(d_logits, w_router, (((1,), (1,)), ((), ())), preferred_element_type=f32)
        grad_tokens = (dx_moe.astype(f32) + router_grad).astype(bf16)
        grad_w_router = lax.psum(jnp.einsum("td,te->de", tokens, d_logits, preferred_element_type=f32), "ep")
        return moe_out, grad_tokens, grad_w_in, grad_w_out, grad_w_router

    in_specs = (row_spec, row_spec, P(None, None), P("ep", None, "tp"), P("ep", "tp", None), P(("dp", "ep")))
    out_specs = (row_spec, row_spec, P(("dp", "ep"), None, "tp"), P(("dp", "ep"), "tp", None), P("dp", None))
    return jax.shard_map(block, mesh=mesh, in_specs=in_specs, out_specs=out_specs, check_vma=False)
```
